32 devices in a mesh: pp: 4 (over x, core), tp: 2 (over y), dp: 4 (over z).
Axes of the slice: x: 2, y: 2, z: 4, core: 2. Of those that a mesh axis runs over, the one named last changes fastest.
Arguments:
- layer_input: bfloat16 [4, 4, 16, 4096], P('pp', 'dp', 'tp'), may hold values from -4 to 4
- gate_pre: bfloat16 [4, 4, 16, 14784], P('pp', 'dp', None, 'tp'), may hold values from -8 to 8
- up_pre: bfloat16 [4, 4, 16, 14784], P('pp', 'dp', None, 'tp'), may hold values from -6 to 6
- hidden_grad: bfloat16 [4, 4, 16, 14784], P('pp', 'dp', None, 'tp'), may hold values from -0.59765625 to 0.59765625
- gate_weight: bfloat16 [4, 4096, 14784], P('pp', 'dp', 'tp'), may hold values from -0.09375 to 0.09375
Outputs:
- passed_grad: bfloat16 [4, 4, 16, 4096], P('pp', 'dp', 'tp')
- gate_weight_grad: bfloat16 [4, 4096, 14784], P('pp', 'dp', 'tp')
The draws below stay inside these ranges and needn't reach their ends.
All inputs are finite; a program needn't handle non-finite values.
Results may differ from the reference program's by a relative error of at most 0.018.
Values may be sent and summed in bfloat16 or wider, within the bound.
No kernel may reach another device: no remote copies, remote signals or barrier semaphores. Data moves between devices by JAX's collectives and lax.ppermute only.
A program may use at most 128 MiB of HBM per device.

```python
import jax
import jax.numpy as jnp
from jax import lax

D = 4096
FF = 14784
GROUP_TOKENS = 16
SECTIONS = 4
REPLICAS = 4
N_PP = 4
N_DP = 4


def spiked(drawn, stream_key, source, target, parts, factor):
    def block_of(dim):
        return (jnp.arange(drawn.shape[dim]) // (drawn.shape[dim] // parts)).reshape((-1,) + (1,) * (drawn.ndim - 1 - dim))

    first = jax.random.permutation(stream_key, parts)[block_of(target)]
    second = (block_of(target) + parts // 2) % parts
    return jnp.where((block_of(source) == first) | (block_of(source) == second), factor * drawn, drawn)


def levels(own_key, extent, pieces, smallest, high):
    loudness = 1.0
    for dim, parts in pieces:
        draws = jax.random.uniform(jax.random.fold_in(jax.random.fold_in(own_key, 6), dim), (parts,), jnp.float32, smallest / len(pieces), high / len(pieces))
        loudness = loudness * jnp.repeat(jnp.exp(draws), extent[dim] // parts).reshape((-1,) + (1,) * (len(extent) - 1 - dim))
    return loudness


def centred(stream_key, extent, width, bound, pieces=(), kind=jnp.bfloat16):
    values = jax.random.normal(stream_key, extent, jnp.float32) * width
    if len(pieces) > 0:
        values = levels(stream_key, extent, pieces, -0.22, 0.18) * values
    return jnp.clip(values, min=-bound, max=bound).astype(kind)


def heavy_noise(rng, shape, scale, limit, cuts, heavy, held_as=jnp.bfloat16):
    result = scale * jax.random.normal(rng, shape, jnp.float32)
    if cuts:
        result = result * levels(rng, shape, cuts, -0.22, 0.18)
    return jnp.clip(spiked(result, jax.random.fold_in(rng, 3), *heavy), -limit, limit).astype(held_as)


def setup_inputs(seed: int = 0) -> dict:
    keys = jax.random.split(jax.random.key(seed), 6)
    layer_input = heavy_noise(keys[0], (SECTIONS, REPLICAS, GROUP_TOKENS, D), 0.5, 4.0, ((0, 4), (1, 4), (2, 2)), (1, 3, 4, 2.0))
    gate_pre = centred(keys[1], (SECTIONS, REPLICAS, GROUP_TOKENS, FF), 1.5, 8.0, ((0, 4), (1, 4), (3, 2)))
    up_pre = centred(keys[2], (SECTIONS, REPLICAS, GROUP_TOKENS, FF), 1.0, 6.0, ((0, 4), (1, 4), (3, 2)))
    hidden_grad = centred(keys[3], (SECTIONS, REPLICAS, GROUP_TOKENS, FF), 0.1, 0.59765625, ((0, 4), (1, 4), (3, 2)))
    gate_weight = centred(keys[4], (SECTIONS, D, FF), D ** -0.5, 0.09375, ((0, 4), (1, 4), (2, 2)))
    return {"layer_input": layer_input, "gate_pre": gate_pre, "up_pre": up_pre, "hidden_grad": hidden_grad, "gate_weight": gate_weight}


def local_grad(gate_act, up_act, hidden):
    gate_val = gate_act.astype(jnp.float32)
    up_val = up_act.astype(jnp.float32)
    hidden_val = hidden.astype(jnp.float32)
    logistic = jax.nn.sigmoid(gate_val)
    return (hidden_val * up_val * logistic * (1.0 + gate_val * (1.0 - logistic))).astype(jnp.bfloat16)

def reference(layer_input, gate_pre, up_pre, hidden_grad, gate_weight):
    input_list = []
    gate_list = []
    for which_section in range(N_PP):
        gate_total = jnp.zeros((D, FF), jnp.float32)
        replica_grads = []
        for replica in range(N_DP):
            gate_grad = local_grad(gate_pre[which_section, replica], up_pre[which_section, replica], hidden_grad[which_section, replica])
            summed = jnp.dot(gate_grad, gate_weight[which_section].T, preferred_element_type=jnp.float32)
            replica_grads.append(summed.astype(jnp.bfloat16))
            tokens_in = layer_input[which_section, replica]
            gate_term = lax.optimization_barrier(jnp.dot(tokens_in.T, gate_grad, preferred_element_type=jnp.float32).astype(jnp.bfloat16))
            gate_total = gate_total + gate_term.astype(jnp.float32)
        input_list.append(jnp.stack(replica_grads))
        gate_list.append(gate_total.astype(jnp.bfloat16))
    zeros_last = jnp.zeros_like(input_list[0])
    passed_grad = jnp.stack(input_list[1:] + [zeros_last])
    return (passed_grad, jnp.stack(gate_list))
```

```python
import jax
import jax.numpy as jnp
from jax import lax
from jax.sharding import PartitionSpec as P


def to_behind(block, axis):
    size = lax.axis_size(axis)
    return lax.ppermute(block, axis, [(i, i - 1) for i in range(1, size)])


def rotated(blocks, start):
    size = blocks.shape[0]
    return lax.dynamic_slice_in_dim(jnp.concatenate([blocks, blocks]), start, size)


def gather_slots(block, axis):
    size = lax.axis_size(axis)
    z = lax.axis_index(axis)
    if size != 4:
        return rotated(lax.all_gather(block, axis), z)
    opposite = lax.ppermute(block, axis, [(i, (i + 2) % 4) for i in range(4)])
    from_low = lax.ppermute(block, axis, [(i, i + 1) for i in range(3)])
    from_high = lax.ppermute(block, axis, [(i + 1, i) for i in range(3)])
    ends = lax.ppermute(opposite, axis, [(2, 3), (1, 0)])
    after = jnp.where(z == 3, ends, from_high)
    before = jnp.where(z == 0, ends, from_low)
    return jnp.stack([block, after, opposite, before])


def on_device(layer_input, gate_pre, up_pre, hidden_grad, gate_weight):
    tokens_in = layer_input[0, 0]
    gate_val = gate_pre[0, 0].astype(jnp.float32)
    up_val = up_pre[0, 0].astype(jnp.float32)
    hidden_val = hidden_grad[0, 0].astype(jnp.float32)
    weight_t = gate_weight[0].T
    dp = lax.axis_size("dp")
    tp = lax.axis_size("tp")
    z = lax.axis_index("dp")
    own, width = tokens_in.shape
    block = width // dp
    tokens = own * tp
    hidden = weight_t.shape[0]
    logistic = jax.nn.sigmoid(gate_val)
    gate_grad = (hidden_val * up_val * logistic * (1.0 + gate_val * (1.0 - logistic))).astype(
        jnp.bfloat16
    )
    grads = gather_slots(gate_grad, "dp").reshape(dp * tokens, hidden)
    split_in = tokens_in.reshape(own, dp, block).transpose(1, 0, 2)
    sent_in = jnp.broadcast_to(split_in[None], (tp, dp, own, block))
    got_in = lax.all_to_all(sent_in.reshape(tp * dp, own, block), ("tp", "dp"), 0, 0, tiled=True)
    got_in = got_in.reshape(tp, dp, own, block).transpose(1, 0, 2, 3).reshape(dp, tokens, block)
    slots_in = rotated(got_in, z).reshape(dp * tokens, block)
    partial_value = jnp.dot(grads, weight_t, preferred_element_type=jnp.float32).astype(jnp.bfloat16)
    by_replica = rotated(partial_value.reshape(dp, tokens, block), (dp - z) % dp)
    to_owner = by_replica.reshape(dp, tp, own, block).transpose(1, 0, 2, 3)
    returned = lax.all_to_all(to_owner.reshape(tp * dp, own, block), ("tp", "dp"), 0, 0, tiled=True)
    summed = jnp.sum(returned.reshape(tp, dp, own, block).astype(jnp.float32), axis=0)
    input_grad = summed.astype(jnp.bfloat16).transpose(1, 0, 2).reshape(own, width)
    passed = to_behind(input_grad, "pp")
    weight_grad_t = lax.dot_general(
        grads, slots_in, (((0,), (0,)), ((), ())), preferred_element_type=jnp.float32
    ).astype(jnp.bfloat16)
    return (passed[None, None], weight_grad_t.T[None])


def solution(mesh):
    return jax.shard_map(
        on_device,
        mesh=mesh,
        in_specs=(
            P("pp", "dp", "tp", None),
            P("pp", "dp", None, "tp"),
            P("pp", "dp", None, "tp"),
            P("pp", "dp", None, "tp"),
            P("pp", "dp", "tp"),
        ),
        out_specs=(P("pp", "dp", "tp", None), P("pp", "dp", "tp")),
        check_vma=False,
    )
```

```python
import jax
import jax.numpy as jnp
from jax import lax
from jax.sharding import PartitionSpec as P


def to_behind(block, axis):
    size = lax.axis_size(axis)
    return lax.ppermute(block, axis, [(i, i - 1) for i in range(1, size)])


def rotated(blocks, start):
    size = blocks.shape[0]
    return lax.dynamic_slice_in_dim(jnp.concatenate([blocks, blocks]), start, size)


def gather_slots(block, axis):
    size = lax.axis_size(axis)
    z = lax.axis_index(axis)
    if size != 4:
        return rotated(lax.all_gather(block, axis), z)
    opposite = lax.ppermute(block, axis, [(i, (i + 2) % 4) for i in range(4)])
    from_low = lax.ppermute(block, axis, [(i, i + 1) for i in range(3)])
    from_high = lax.ppermute(block, axis, [(i + 1, i) for i in range(3)])
    ends = lax.ppermute(opposite, axis, [(2, 3), (1, 0)])
    after = jnp.where(z == 3, ends, from_high)
    before = jnp.where(z == 0, ends, from_low)
    return jnp.stack([block, after, opposite, before])


def on_device(layer_input, gate_pre, up_pre, hidden_grad, gate_weight):
    tokens_in = layer_input[0, 0]
    gate_val = gate_pre[0, 0].astype(jnp.float32)
    up_val = up_pre[0, 0].astype(jnp.float32)
    hidden_val = hidden_grad[0, 0].astype(jnp.float32)
    weight_t = gate_weight[0].T
    dp = lax.axis_size("dp")
    tp = lax.axis_size("tp")
    z = lax.axis_index("dp")
    own, width = tokens_in.shape
    block = width // dp
    tokens = own * tp
    hidden = weight_t.shape[0]
    logistic = jax.nn.sigmoid(gate_val)
    gate_grad = (hidden_val * up_val * logistic * (1.0 + gate_val * (1.0 - logistic))).astype(
        jnp.bfloat16
    )
    grads = gather_slots(gate_grad, "dp").reshape(dp * tokens, hidden)
    split_in = tokens_in.reshape(own, dp, block).transpose(1, 0, 2)
    sent_in = jnp.broadcast_to(split_in[None], (tp, dp, own, block))
    got_in = lax.all_to_all(sent_in.reshape(tp * dp, own, block), ("tp", "dp"), 0, 0, tiled=True)
    got_in = got_in.reshape(tp, dp, own, block).transpose(1, 0, 2, 3).reshape(dp, tokens, block)
    slots_in = rotated(got_in, z).reshape(dp * tokens, block)
    partial_value = jnp.dot(grads, weight_t, preferred_element_type=jnp.float32).astype(jnp.bfloat16)
    by_replica = rotated(partial_value.reshape(dp, tokens, block), (dp - z) % dp)
    to_owner = by_replica.reshape(dp, tp, own, block).transpose(1, 0, 2, 3)
    returned = lax.all_to_all(to_owner.reshape(tp * dp, own, block), ("tp", "dp"), 0, 0, tiled=True)
    weight_grad_t = lax.dot_general(
        grads, slots_in, (((0,), (0,)), ((), ())), preferred_element_type=jnp.float32
    ).astype(jnp.bfloat16)
    returned, weight_grad_t = lax.optimization_barrier((returned, weight_grad_t))
    summed = jnp.sum(returned.reshape(tp, dp, own, block).astype(jnp.float32), axis=0)
    input_grad = summed.astype(jnp.bfloat16).transpose(1, 0, 2).reshape(own, width)
    passed = to_behind(input_grad, "pp")
    return (passed[None, None], weight_grad_t.T[None])


def solution(mesh):
    return jax.shard_map(
        on_device,
        mesh=mesh,
        in_specs=(
            P("pp", "dp", "tp", None),
            P("pp", "dp", None, "tp"),
            P("pp", "dp", None, "tp"),
            P("pp", "dp", None, "tp"),
            P("pp", "dp", "tp"),
        ),
        out_specs=(P("pp", "dp", "tp", None), P("pp", "dp", "tp")),
        check_vma=False,
    )
```
